32 devices in a mesh: seq: 8 (over z, x), head: 4 (over y, core).
Axes of the slice: x: 2, y: 2, z: 4, core: 2. Of those that a mesh axis runs over, the one named last changes fastest.
Arguments:
- c_query: bfloat16 [256, 1536], P('seq', 'head'), may hold values from -60 to 60
- q_gain: float32 [1536], replicated, may hold values from 0.25 to 1.75
- w_query: bfloat16 [1536, 12288], P(None, 'head'), may hold values from -0.15625 to 0.15625
- kv_latent: bfloat16 [4096, 576], P('seq'), may hold values from -800 to 800
- kv_gain: float32 [512], replicated, may hold values from 0.25 to 1.75
- w_kv: bfloat16 [512, 16384], P(None, ('head', 'seq')), may hold values from -0.25 to 0.25
- w_out: bfloat16 [8192, 7168], P('head', 'seq'), may hold values from -0.5 to 0.5
- q_start: int32 [256], P('seq'), may hold values from 0 to 4095, as said below
Outputs:
- out: bfloat16 [256, 7168], P('head', 'seq')
The draws below stay inside these ranges and needn't reach their ends.
Inputs may be any that keep to these rules, and one draw needn't show every extreme that they name: q_start[i] is at most pos_i and at least 512 * (i // 32 - 3); in every draw some query's q_start equals that lower limit. Within a block of 32 queries q_start never falls.
All inputs are finite; a program needn't handle non-finite values.
Results may differ from the reference program's by a relative error of at most 0.018.
The reference program's roundings to bfloat16 on the way count: a program that leaves them out, or rounds other values in their place, can miss the bound.
Values may be sent and summed in bfloat16 or wider, within the bound.
No kernel may reach another device: no remote copies, remote signals or barrier semaphores. Data moves between devices by JAX's collectives and lax.ppermute only.
A program may use at most 128 MiB of HBM per device.

```python
import jax
import jax.numpy as jnp
from jax import lax

D = 7168
QL = 1536
KVL = 512
NOPE = 128
ROPE = 64
VDIM = 128
H = 64
REACH = 3
KEY_DEV = 512
QRY_DEV = 32
KEYS = 4096
QUERIES = 256


def draw_c_query(key, part):
    key_base = jax.random.fold_in(jax.random.fold_in(key, 7), 0)
    drawn_values = jnp.clip(jax.random.normal(key_base, (QUERIES, QL), jnp.float32), -6.0, 6.0)
    return drawn_values.astype(jnp.bfloat16)


def draw_kv_latent(key, part):
    key_base = jax.random.fold_in(jax.random.fold_in(key, 23), 0)
    drawn_values = jnp.clip(jax.random.normal(key_base, (KEYS, KVL + ROPE), jnp.float32), -6.0, 6.0)
    return drawn_values.astype(jnp.bfloat16)


def draw_q_start(key, part):
    key_far, key_pick, key_cut, key_late = jax.random.split(jax.random.fold_in(key, 31), 4)
    block_count = QUERIES // QRY_DEV
    block_ids = jnp.arange(block_count, dtype=jnp.int32)
    window_first = block_ids * KEY_DEV + KEY_DEV - QRY_DEV
    lower = (block_ids - REACH) * KEY_DEV
    far = lower + jax.random.randint(key_far, (block_count,), 0, KEY_DEV // 2 + 1, dtype=jnp.int32)
    chosen = jax.random.randint(key_pick, (), REACH, block_count, dtype=jnp.int32)
    far = jnp.where(block_ids == chosen, lower, far)
    far = jnp.maximum(far, 0)
    cut = jax.random.randint(key_cut, (block_count,), 1, QRY_DEV, dtype=jnp.int32)
    final_block = block_ids == block_count - 1
    cut = jnp.where(final_block, QRY_DEV - 1, cut)
    late_room = window_first + cut - far + 1
    late = far + jax.random.randint(key_late, (block_count,), 0, 1 << 20, dtype=jnp.int32) % late_room
    late = jnp.where(final_block, window_first + QRY_DEV - 1, late)
    serial = jnp.arange(QUERIES, dtype=jnp.int32)
    block_of = serial // QRY_DEV
    inner = serial % QRY_DEV
    starts = jnp.where(inner[:, None] < cut[None, :], far[None, :], late[None, :])
    pick = (block_of[:, None] == block_ids[None, :]).astype(jnp.int32)
    return jnp.sum(starts * pick, axis=1).astype(jnp.int32)


def block_levels(stream_key, extent, cuts, least, high):
    loudness = 1.0
    for axis_at, parts in cuts:
        draws = jax.random.uniform(jax.random.fold_in(jax.random.fold_in(stream_key, 6), axis_at), (parts,), jnp.float32, least / len(cuts), high / len(cuts))
        loudness = loudness * jnp.repeat(jnp.exp(draws), extent[axis_at] // parts).reshape((-1,) + (1,) * (len(extent) - 1 - axis_at))
    return loudness


def scatter_about(rng, dims, spread, limit, shards=(), held_as=jnp.bfloat16):
    array = spread * jax.random.normal(rng, dims, jnp.float32)
    if shards:
        array = array * block_levels(rng, dims, shards, -0.22, 0.18)
    return jnp.clip(array, -limit, limit).astype(held_as)


def setup_inputs(seed: int = 0) -> dict:
    key_list = jax.random.split(jax.random.key(seed), 9)
    return {
        "c_query": draw_c_query(jax.random.fold_in(key_list[8], 71), 0),
        "q_gain": jnp.clip(1.0 + 0.15 * jax.random.normal(key_list[1], (QL,), jnp.float32), 0.25, 1.75),
        "w_query": scatter_about(key_list[2], (QL, H * (NOPE + ROPE)), QL ** -0.5, 0.15625, ((1, 4),)),
        "kv_latent": draw_kv_latent(jax.random.fold_in(key_list[8], 71), 0),
        "kv_gain": jnp.clip(1.0 + 0.15 * jax.random.normal(key_list[4], (KVL,), jnp.float32), 0.25, 1.75),
        "w_kv": scatter_about(key_list[5], (KVL, H * (NOPE + VDIM)), KVL ** -0.5, 0.25, ((1, 32),)),
        "w_out": scatter_about(key_list[6], (H * VDIM, D), VDIM ** -0.5, 0.5, ((0, 4), (1, 8))),
        "q_start": draw_q_start(jax.random.fold_in(key_list[8], 71), 0),
    }


EPS = 1e-06
THETA = 10000.0
PRECISE = lax.Precision.HIGHEST

def rms_scale(latent_rows, gain_row):
    values = latent_rows.astype(jnp.float32)
    mean_square = lax.optimization_barrier(jnp.mean(values * values, axis=-1, keepdims=True))
    return values * lax.rsqrt(mean_square + EPS) * gain_row

def rotate(rotary, position):
    half_size = rotary.shape[-1] // 2
    exponent = jnp.arange(half_size, dtype=jnp.float32) * (2.0 / rotary.shape[-1])
    angles = position.astype(jnp.float32)[:, None] * (THETA ** (-exponent))[None, :]
    cosine = jnp.cos(angles)[:, None, :]
    sine_of = jnp.sin(angles)[:, None, :]
    former = rotary[..., :half_size]
    latter = rotary[..., half_size:]
    return jnp.concatenate([former * cosine - latter * sine_of, latter * cosine + former * sine_of], axis=-1)

def reference(c_query, q_gain, w_query, kv_latent, kv_gain, w_kv, w_out, q_start):
    queries = c_query.shape[0]
    blocks = queries // QRY_DEV
    head_count = w_query.shape[1] // (NOPE + ROPE)
    window_blocks = REACH + 1
    normed = rms_scale(c_query, q_gain).astype(jnp.bfloat16)
    query_raw = jnp.dot(normed, w_query, preferred_element_type=jnp.float32).reshape(queries, head_count, NOPE + ROPE)
    serial = jnp.arange(queries, dtype=jnp.int32)
    position = serial // QRY_DEV * KEY_DEV + KEY_DEV - QRY_DEV + serial % QRY_DEV
    query_all = jnp.concatenate([query_raw[..., :NOPE], rotate(query_raw[..., NOPE:], position)], axis=-1).astype(jnp.bfloat16)

    def project(latent_block):
        scaled = rms_scale(latent_block, kv_gain).astype(jnp.bfloat16)
        return jnp.dot(scaled, w_kv, preferred_element_type=jnp.float32).astype(jnp.bfloat16)
    latent_blocks = kv_latent[:, :KVL].reshape(blocks, KEY_DEV, KVL)
    head_blocks = lax.map(project, latent_blocks)
    head_blocks = jnp.concatenate([jnp.zeros((REACH, KEY_DEV, head_blocks.shape[2]), jnp.bfloat16), head_blocks], axis=0)
    rope_blocks = kv_latent[:, KVL:].reshape(blocks, KEY_DEV, ROPE)
    rope_blocks = jnp.concatenate([jnp.zeros((REACH, KEY_DEV, ROPE), jnp.bfloat16), rope_blocks], axis=0)
    query_blocks = query_all.reshape(blocks, QRY_DEV, head_count, NOPE + ROPE)
    start_blocks = q_start.reshape(blocks, QRY_DEV)
    place_blocks = position.reshape(blocks, QRY_DEV)

    def attend(block_index):
        window = lax.dynamic_slice_in_dim(head_blocks, block_index, window_blocks, 0)
        window = window.reshape(window_blocks * KEY_DEV, head_count, NOPE + VDIM).astype(jnp.float32)
        rope_keys = lax.dynamic_slice_in_dim(rope_blocks, block_index, window_blocks, 0)
        rope_keys = rope_keys.reshape(window_blocks * KEY_DEV, ROPE).astype(jnp.float32)
        query_here = lax.dynamic_index_in_dim(query_blocks, block_index, 0, keepdims=False).astype(jnp.float32)
        starts = lax.dynamic_index_in_dim(start_blocks, block_index, 0, keepdims=False)
        places = lax.dynamic_index_in_dim(place_blocks, block_index, 0, keepdims=False)
        key_place = (block_index - REACH) * KEY_DEV + jnp.arange(window_blocks * KEY_DEV, dtype=jnp.int32)
        scores = jnp.einsum('qhd,khd->hqk', query_here[..., :NOPE], window[..., :NOPE], precision=PRECISE)
        scores = scores + jnp.einsum('qhd,kd->hqk', query_here[..., NOPE:], rope_keys, precision=PRECISE)
        scores = scores * (NOPE + ROPE) ** (-0.5)
        allowed = (key_place[None, :] >= starts[:, None]) & (key_place[None, :] <= places[:, None])
        scores = jnp.where(allowed[None], scores, -jnp.inf)
        largest = lax.optimization_barrier(jnp.max(scores, axis=-1, keepdims=True))
        exponent_terms = jnp.exp(scores - largest)
        weights_bf = (exponent_terms / lax.optimization_barrier(jnp.sum(exponent_terms, axis=-1, keepdims=True))).astype(jnp.bfloat16)
        weights_wide = lax.optimization_barrier(weights_bf).astype(jnp.float32)
        attended = jnp.einsum('hqk,khd->qhd', weights_wide, window[..., NOPE:], precision=PRECISE)
        return attended.astype(jnp.bfloat16).reshape(QRY_DEV, head_count * VDIM)
    attended_all = lax.map(attend, jnp.arange(blocks, dtype=jnp.int32)).reshape(queries, head_count * VDIM)
    return jnp.dot(attended_all, w_out, preferred_element_type=jnp.float32).astype(jnp.bfloat16)
```

```python
import functools

import jax
import jax.numpy as jnp
from jax import lax
from jax.experimental import pallas as pl
from jax.experimental.pallas import tpu as pltpu
from jax.sharding import PartitionSpec as P

KVL = 512
NOPE = 128
ROPE = 64
VDIM = 128
REACH = 3
DIGIT = 64


EPS = 1e-06
THETA = 10000.0


def passed_along(x, axis, by):
    devices = lax.axis_size(axis)
    pairs = [(i, i + by) for i in range(devices) if 0 <= i + by < devices]
    return lax.ppermute(x, axis, pairs)


def rms_scale(latent_rows, gain_row):
    values = latent_rows.astype(jnp.float32)
    mean_square = jnp.mean(values * values, axis=-1, keepdims=True)
    return values * lax.rsqrt(mean_square + EPS) * gain_row


def rotate(rotary, position):
    half_size = rotary.shape[-1] // 2
    exponent = jnp.arange(half_size, dtype=jnp.float32) * (2.0 / rotary.shape[-1])
    angles = position.astype(jnp.float32)[:, None] * (THETA ** (-exponent))[None, :]
    cosine = jnp.cos(angles)[:, None, :]
    sine_of = jnp.sin(angles)[:, None, :]
    former = rotary[..., :half_size]
    latter = rotary[..., half_size:]
    return jnp.concatenate(
        [former * cosine - latter * sine_of, latter * cosine + former * sine_of], axis=-1
    )


def masked_scores(query_block, starts, places, key_heads, rope_keys, first_key):
    key_place = first_key + jnp.arange(key_heads.shape[0], dtype=jnp.int32)
    scores = jnp.einsum(
        "qhd,khd->hqk",
        query_block[..., :NOPE],
        key_heads[..., :NOPE],
        preferred_element_type=jnp.float32,
    )
    scores = scores + jnp.einsum(
        "qhd,kd->hqk", query_block[..., NOPE:], rope_keys, preferred_element_type=jnp.float32
    )
    scores = scores * (NOPE + ROPE) ** (-0.5)
    allowed = (key_place[None, :] >= starts[:, None]) & (key_place[None, :] <= places[:, None])
    return (jnp.where(allowed[None], scores, -jnp.inf), allowed)


def body(c_query, q_gain, w_query, kv_latent, kv_gain, w_kv, w_out, q_start):
    query_rows = c_query.shape[0]
    key_rows = kv_latent.shape[0]
    head_count = w_query.shape[1] // (NOPE + ROPE)
    block_index = lax.axis_index("seq")
    full_query = lax.all_gather(c_query, "head", axis=1, tiled=True)
    normed = rms_scale(full_query, q_gain).astype(jnp.bfloat16)
    query_raw = jnp.dot(normed, w_query, preferred_element_type=jnp.float32).reshape(
        query_rows, head_count, NOPE + ROPE
    )
    position = (
        block_index * key_rows + key_rows - query_rows + jnp.arange(query_rows, dtype=jnp.int32)
    )
    query_all = jnp.concatenate(
        [query_raw[..., :NOPE], rotate(query_raw[..., NOPE:], position)], axis=-1
    ).astype(jnp.bfloat16)
    kv_weights = lax.all_gather(w_kv, "seq", axis=1, tiled=True)

    def project(latent_block):
        scaled = rms_scale(latent_block, kv_gain).astype(jnp.bfloat16)
        return jnp.dot(scaled, kv_weights, preferred_element_type=jnp.float32).astype(jnp.bfloat16)

    own_heads = project(kv_latent[:, :KVL])
    own_rope = kv_latent[:, KVL:]
    head_parts = [own_heads]
    rope_parts = [own_rope]
    for offset in range(1, REACH + 1):
        moved_block = passed_along(kv_latent, "seq", offset)
        head_parts.insert(0, project(moved_block[:, :KVL]))
        rope_parts.insert(0, moved_block[:, KVL:])
    window_blocks = REACH + 1
    key_heads = jnp.concatenate(head_parts, axis=0).reshape(
        window_blocks * key_rows, head_count, NOPE + VDIM
    )
    rope_keys = jnp.concatenate(rope_parts, axis=0)
    scores, allowed = masked_scores(
        query_all, q_start, position, key_heads, rope_keys, (block_index - REACH) * key_rows
    )
    largest = jnp.max(scores, axis=-1, keepdims=True)
    exponent_terms = jnp.exp(scores - largest)
    weights_bf = (exponent_terms / jnp.sum(exponent_terms, axis=-1, keepdims=True)).astype(
        jnp.bfloat16
    )
    attended = jnp.einsum(
        "hqk,khd->qhd", weights_bf, key_heads[..., NOPE:], preferred_element_type=jnp.float32
    )
    attended = attended.astype(jnp.bfloat16).reshape(query_rows, head_count * VDIM)
    partial_rows = jnp.dot(
        lax.all_gather(attended, "seq", axis=0, tiled=True),
        w_out,
        preferred_element_type=jnp.float32,
    )
    return lax.psum_scatter(partial_rows, "head", scatter_dimension=0, tiled=True).astype(
        jnp.bfloat16
    )


def exchanged(x, axis, flip):
    pairs = [(i, i ^ flip) for i in range(lax.axis_size(axis))]
    return lax.ppermute(x, axis, pairs)


def pack_kernel(place_ref, start_ref, latent_ref, gain_ref, query_ref, packed_ref):
    rows = latent_ref.shape[0]
    half = KVL // 2
    values = latent_ref[:, :KVL].astype(jnp.float32)
    mean_square = jnp.mean(values * values, axis=-1, keepdims=True)
    normed = (values * lax.rsqrt(mean_square + EPS) * gain_ref[...]).astype(jnp.bfloat16)
    packed_ref[:rows, :] = normed[:, :half]
    packed_ref[rows : 2 * rows, :] = normed[:, half:]
    rope = latent_ref[:, KVL:]
    quarter = rows // 4
    at = 2 * rows
    packed_ref[at : at + quarter, :] = jnp.concatenate(
        [rope[g * quarter : (g + 1) * quarter] for g in range(4)], axis=1
    )
    at += quarter
    query_rows = query_ref.shape[0]
    packed_ref[at : at + query_rows, :] = query_ref[:, :half]
    at += query_rows
    folded = query_rows // 2
    packed_ref[at : at + folded, :] = jnp.concatenate(
        [query_ref[:folded, half:], query_ref[folded:, half:]], axis=1
    )
    at += folded
    share = packed_ref.shape[0] - at
    window_first = (place_ref[0] - REACH) * (rows * (query_rows // share))
    shape = (share, half)
    row = lax.broadcasted_iota(jnp.int32, shape, 0)
    offset = jnp.zeros(shape, jnp.int32)
    for r in range(share):
        offset = jnp.where(row == r, start_ref[place_ref[1] * share + r] - window_first, offset)
    high = offset // DIGIT
    digit = jnp.where(
        lax.broadcasted_iota(jnp.int32, shape, 1) < half // 2, high, offset - high * DIGIT
    )
    packed_ref[at:, :] = digit.astype(jnp.float32).astype(jnp.bfloat16)


def pack(place, kv_latent, kv_gain, c_query, q_start):
    head_devices = lax.axis_size("head")
    rows = kv_latent.shape[0] // head_devices
    query_rows = c_query.shape[0]
    packed_rows = 2 * rows + rows // 4 + query_rows + query_rows // 2 + query_rows // head_devices
    return pl.pallas_call(
        pack_kernel,
        out_shape=jax.ShapeDtypeStruct((packed_rows, KVL // 2), jnp.bfloat16),
        grid_spec=pltpu.PrefetchScalarGridSpec(
            num_scalar_prefetch=2,
            grid=(1,),
            in_specs=[
                pl.BlockSpec((rows, KVL + ROPE), lambda i, p, q: (p[1], 0)),
                pl.BlockSpec((1, KVL), lambda i, p, q: (0, 0)),
                pl.BlockSpec(c_query.shape, lambda i, p, q: (0, 0)),
            ],
            out_specs=pl.BlockSpec((packed_rows, KVL // 2), lambda i, p, q: (0, 0)),
        ),
        name="pack",
    )(place, q_start, kv_latent, kv_gain.reshape(1, KVL), c_query)


def gather_pieces(own):
    along_z = lambda v, k: exchanged(v, "seq", 2 * k)
    along_x = lambda v: exchanged(v, "seq", 1)
    along_y = lambda v: exchanged(v, "head", 2)
    got = {(0, 0): own}
    for k in (1, 2, 3):
        got[2 * k, 0] = along_z(own, k)
    for k in (0, 1, 2, 3):
        here = got[2 * k, 0]
        over_x = got[2 * k + 1, 0] = along_x(here)
        over_y = got[2 * k, 2] = along_y(here)
        got[2 * k + 1, 2] = along_x(over_y) if k % 2 else along_y(over_x)
    for (seq_flip, head_flip), v in list(got.items()):
        got[seq_flip, head_flip + 1] = exchanged(v, "head", 1)
    return got


def attend_kernel(flips, blocks, place_ref, *refs):
    pieces = refs[: len(flips)]
    (w_query_ref, w_kv_ref, gain_ref, cos_ref, sin_ref, out_ref) = refs[
        len(flips) : len(flips) + 6
    ]
    (packs, w_query, latent_query, queries, keys, values, scores, probs, sems) = refs[
        len(flips) + 6 :
    ]
    seq_at = place_ref[0]
    head_at = place_ref[1]
    parts = len(flips) // blocks
    heads = queries.shape[0]
    wide = NOPE + ROPE
    query_rows = queries.shape[1] // blocks
    key_rows = keys.shape[1] // blocks
    rows = key_rows // parts
    half = KVL // 2
    weight_copy = pltpu.make_async_copy(
        w_query_ref.at[:, pl.ds(pl.multiple_of(seq_at * (heads * wide), 128), heads * wide)],
        w_query,
        sems.at[len(flips)],
    )
    weight_copy.start()
    for piece, (seq_flip, head_flip) in zip(pieces, flips):
        to = (seq_at ^ seq_flip) * parts + (head_at ^ head_flip)
        pltpu.make_async_copy(piece, packs.at[to], sems.at[to]).start()

    rope_at = 2 * rows
    query_at = rope_at + rows // 4
    fold_at = query_at + query_rows
    folded = query_rows // 2
    start_at = fold_at + folded
    query_wide = latent_query.shape[1] // parts
    for b in range(blocks):
        for part in range(parts):
            to = b * parts + part
            pltpu.make_async_copy(pieces[0], packs.at[to], sems.at[to]).wait()
    for b in range(blocks):
        for part in range(parts):
            to = b * parts + part
            at = part * query_wide
            top = b * query_rows
            latent_query[top : top + query_rows, at : at + half] = packs[
                to, query_at : query_at + query_rows, :
            ]
            rest = query_wide - half
            for f in range(2):
                latent_query[
                    top + f * folded : top + (f + 1) * folded, at + half : at + query_wide
                ] = packs[to, fold_at : fold_at + folded, f * rest : (f + 1) * rest]
    weight_copy.wait()
    for b in range(blocks):
        top = b * query_rows
        span = slice(top, top + query_rows)
        wide_rows = latent_query[span, :].astype(jnp.float32)
        mean_square = jnp.mean(wide_rows * wide_rows, axis=-1, keepdims=True)
        latent_query[span, :] = (
            wide_rows * lax.rsqrt(mean_square + EPS) * gain_ref[...]
        ).astype(jnp.bfloat16)
    raw = jnp.dot(latent_query[...], w_query[...], preferred_element_type=jnp.float32)
    for j in range(heads):
        head_raw = raw[:, j * wide : (j + 1) * wide]
        queries[j, :, :NOPE] = head_raw[:, :NOPE].astype(jnp.bfloat16)
        rotary = head_raw[:, NOPE:]
        crossed = jnp.concatenate([rotary[:, ROPE // 2 :], rotary[:, : ROPE // 2]], axis=1)
        queries[j, :, NOPE:] = (rotary * cos_ref[...] + crossed * sin_ref[...]).astype(
            jnp.bfloat16
        )

    def project(b):
        for part in range(parts):
            to = b * parts + part
            top = b * key_rows + part * rows
            both = jnp.dot(
                packs[to, :rows, :], w_kv_ref[:half, :], preferred_element_type=jnp.float32
            ) + jnp.dot(
                packs[to, rows : 2 * rows, :],
                w_kv_ref[half:, :],
                preferred_element_type=jnp.float32,
            )
            both = both.astype(jnp.bfloat16)
            quarter = rows // 4
            for j in range(heads):
                left = j * (NOPE + VDIM)
                keys[j, top : top + rows, :NOPE] = both[:, left : left + NOPE]
                values[j, top : top + rows, :] = both[:, left + NOPE : left + NOPE + VDIM]
                for g in range(4):
                    keys[j, top + g * quarter : top + (g + 1) * quarter, NOPE:] = packs[
                        to, rope_at : rope_at + quarter, g * ROPE : (g + 1) * ROPE
                    ]

    def score(b):
        count = min(REACH + 1, blocks - b) * query_rows
        for j in range(heads):
            scores[j, b, :count, :] = lax.dot_general(
                queries[j, b * query_rows : b * query_rows + count, :],
                keys[j, b * key_rows : (b + 1) * key_rows, :],
                (((1,), (1,)), ((), ())),
                preferred_element_type=jnp.float32,
            )

    def soften(b):
        digits = jnp.concatenate(
            [packs[b * parts + part, start_at:, :].astype(jnp.float32) for part in range(parts)],
            axis=0,
        )
        offset = digits[:, :128] * DIGIT + digits[:, half // 2 : half // 2 + 128]
        start = jnp.concatenate([offset] * (key_rows // 128), axis=1).astype(jnp.int32)
        window = range(max(b - REACH, 0), b + 1)
        shape = (query_rows, key_rows)
        column = lax.broadcasted_iota(jnp.int32, shape, 1)
        row = lax.broadcasted_iota(jnp.int32, shape, 0)
        for j in range(heads):
            masked = []
            for w in window:
                top = (b - w) * query_rows
                part = scores[j, w, top : top + query_rows, :] * wide ** (-0.5)
                allowed = column >= start - (w - b + REACH) * key_rows
                if w == b:
                    allowed = allowed & (column <= row + (key_rows - query_rows))
                masked.append(jnp.where(allowed, part, -jnp.inf))
            largest = masked[0]
            for part in masked[1:]:
                largest = jnp.maximum(largest, part)
            largest = jnp.max(largest, axis=-1, keepdims=True)
            terms = [jnp.exp(part - largest) for part in masked]
            total = terms[0]
            for part in terms[1:]:
                total = total + part
            inverse = 1.0 / jnp.sum(total, axis=-1, keepdims=True)
            for w, part in zip(window, terms):
                top = (b - w) * query_rows
                probs[j, w, top : top + query_rows, :] = (part * inverse).astype(jnp.bfloat16)

    for b in range(blocks):
        project(b)
        score(b)
        soften(b)
    for j in range(heads):
        sums = [None] * blocks
        for w in range(blocks):
            count = min(REACH + 1, blocks - w)
            mixed = jnp.dot(
                probs[j, w, : count * query_rows, :],
                values[j, w * key_rows : (w + 1) * key_rows, :],
                preferred_element_type=jnp.float32,
            )
            for i in range(count):
                part = mixed[i * query_rows : (i + 1) * query_rows]
                sums[w + i] = part if sums[w + i] is None else sums[w + i] + part
            out_ref[w * query_rows : (w + 1) * query_rows, j * VDIM : (j + 1) * VDIM] = sums[
                w
            ].astype(jnp.bfloat16)


def attend(place, got, w_query, w_kv, q_gain, cosine, sine_of, query_rows, key_rows):
    blocks = lax.axis_size("seq")
    flips = tuple(sorted(got))
    pieces = [got[f] for f in flips]
    heads = w_kv.shape[1] // (NOPE + VDIM)
    wide = NOPE + ROPE
    queries = blocks * query_rows
    keys = key_rows * blocks
    count = (REACH + 1) * query_rows
    any_spec = pl.BlockSpec(memory_space=pl.ANY)
    vmem = pl.BlockSpec(memory_space=pltpu.VMEM)
    return pl.pallas_call(
        functools.partial(attend_kernel, flips, blocks),
        out_shape=jax.ShapeDtypeStruct((queries, heads * VDIM), jnp.bfloat16),
        in_specs=[pl.BlockSpec(memory_space=pltpu.SMEM)]
        + [any_spec] * (len(flips) + 1)
        + [vmem] * 4,
        out_specs=vmem,
        scratch_shapes=[
            pltpu.VMEM((len(flips),) + pieces[0].shape, jnp.bfloat16),
            pltpu.VMEM((w_query.shape[0], heads * wide), jnp.bfloat16),
            pltpu.VMEM((queries, w_query.shape[0]), jnp.bfloat16),
            pltpu.VMEM((heads, queries, wide), jnp.bfloat16),
            pltpu.VMEM((heads, keys, wide), jnp.bfloat16),
            pltpu.VMEM((heads, keys, VDIM), jnp.bfloat16),
            pltpu.VMEM((heads, blocks, count, key_rows), jnp.float32),
            pltpu.VMEM((heads, blocks, count, key_rows), jnp.bfloat16),
            pltpu.SemaphoreType.DMA((len(flips) + 1,)),
        ],
        name="attend",
    )(place, *pieces, w_query, w_kv, q_gain.reshape(1, -1), cosine, sine_of)


def project_out_kernel(blocks, place_ref, *refs):
    pieces = refs[:blocks]
    w_out_ref = refs[blocks]
    outs = refs[blocks + 1 : -1]
    summed = refs[-1]
    seq_at = place_ref[0]
    head_at = place_ref[1]
    features = pieces[0].shape[1]
    columns = w_out_ref.shape[1]
    for left in range(0, columns, 256):
        span = slice(left, min(left + 256, columns))
        total = None
        for flip in range(blocks):
            top = pl.multiple_of((seq_at ^ flip) * features, features)
            part = jnp.dot(
                pieces[flip][...],
                w_out_ref[pl.ds(top, features), span],
                preferred_element_type=jnp.float32,
            )
            total = part if total is None else total + part
        summed[:, span] = total
    rows = outs[0].shape[0]
    for flip, out_ref in enumerate(outs):
        top = pl.multiple_of((head_at ^ flip) * rows, rows)
        out_ref[...] = summed[pl.ds(top, rows), :].astype(out_ref.dtype)


def project_out(place, pieces, w_out):
    owners = lax.axis_size("head")
    queries = pieces[0].shape[0]
    columns = w_out.shape[1]
    vmem = pl.BlockSpec(memory_space=pltpu.VMEM)
    return pl.pallas_call(
        functools.partial(project_out_kernel, len(pieces)),
        out_shape=[
            jax.ShapeDtypeStruct((queries // owners, columns), jnp.bfloat16 if k else jnp.float32)
            for k in range(owners)
        ],
        in_specs=[pl.BlockSpec(memory_space=pltpu.SMEM)] + [vmem] * (len(pieces) + 1),
        out_specs=[vmem] * owners,
        scratch_shapes=[pltpu.VMEM((queries, columns), jnp.float32)],
        name="project_out",
    )(place, *pieces, w_out)


def heads_body(c_query, q_gain, w_query, kv_latent, kv_gain, w_kv, w_out, q_start):
    blocks = lax.axis_size("seq")
    query_rows = c_query.shape[0]
    key_rows = kv_latent.shape[0]
    seq_at = lax.axis_index("seq")
    head_at = lax.axis_index("head")
    place = jnp.stack([seq_at, head_at]).astype(jnp.int32)
    own = pack(place, kv_latent, kv_gain, c_query, q_start)
    got = gather_pieces(own)
    serial = jnp.arange(blocks * query_rows, dtype=jnp.int32)
    position = serial // query_rows * key_rows + key_rows - query_rows + serial % query_rows
    exponent = jnp.arange(ROPE // 2, dtype=jnp.float32) * (2.0 / ROPE)
    angles = position.astype(jnp.float32)[:, None] * (THETA ** (-exponent))[None, :]
    cosine = jnp.cos(angles)
    sine_of = jnp.sin(angles)
    cosine = jnp.concatenate([cosine, cosine], axis=1)
    sine_of = jnp.concatenate([-sine_of, sine_of], axis=1)
    attended = attend(place, got, w_query, w_kv, q_gain, cosine, sine_of, query_rows, key_rows)
    spread = {0: attended}
    spread[1] = exchanged(attended, "seq", 1)
    for k in (2, 4, 6):
        spread[k] = exchanged(attended, "seq", k)
    spread[3] = exchanged(spread[1], "seq", 2)
    spread[5] = exchanged(spread[4], "seq", 1)
    spread[7] = exchanged(spread[6], "seq", 1)
    shares = project_out(place, [spread[k] for k in range(blocks)], w_out)
    total = shares[0]
    for k in (1, 2, 3):
        total = total + exchanged(shares[k], "head", k).astype(jnp.float32)
    return total.astype(jnp.bfloat16)


def solution(mesh):
    in_specs = (
        P("seq", "head"),
        P(),
        P(None, "head"),
        P("seq", None),
        P(),
        P(None, ("head", "seq")),
        P("head", "seq"),
        P("seq"),
    )
    out_specs = P("head", "seq")

    def layer(*args):
        c_query, _, w_query, kv_latent, _, w_kv, _, _ = args
        seq, heads = mesh.shape["seq"], mesh.shape["head"]
        own_columns = w_kv.shape[1] // (seq * heads)
        whole_heads = own_columns % (NOPE + VDIM) == 0
        by_heads = whole_heads and (seq, heads) == (8, 4)
        step = jax.shard_map(
            heads_body if by_heads else body,
            mesh=mesh,
            in_specs=in_specs,
            out_specs=out_specs,
            check_vma=False,
        )
        return step(*args)

    return layer
```

```python
import functools

import jax
import jax.numpy as jnp
import numpy as np
from jax import lax
from jax.experimental import pallas as pl
from jax.experimental.pallas import tpu as pltpu
from jax.sharding import PartitionSpec as P


KVL = 512
NOPE = 128
ROPE = 64
VDIM = 128
REACH = 3
DIGIT = 64
STAGE_LIMIT = 52000 << 10


EPS = 1e-06
THETA = 10000.0


def passed_along(x, axis, by):
    devices = lax.axis_size(axis)
    pairs = [(i, i + by) for i in range(devices) if 0 <= i + by < devices]
    return lax.ppermute(x, axis, pairs)


def rms_scale(latent_rows, gain_row):
    values = latent_rows.astype(jnp.float32)
    mean_square = jnp.mean(values * values, axis=-1, keepdims=True)
    return values * lax.rsqrt(mean_square + EPS) * gain_row


def rotate(rotary, position):
    half_size = rotary.shape[-1] // 2
    exponent = jnp.arange(half_size, dtype=jnp.float32) * (2.0 / rotary.shape[-1])
    angles = position.astype(jnp.float32)[:, None] * (THETA ** (-exponent))[None, :]
    cosine = jnp.cos(angles)[:, None, :]
    sine_of = jnp.sin(angles)[:, None, :]
    former = rotary[..., :half_size]
    latter = rotary[..., half_size:]
    return jnp.concatenate(
        [former * cosine - latter * sine_of, latter * cosine + former * sine_of], axis=-1
    )


def masked_scores(query_block, starts, places, key_heads, rope_keys, first_key):
    key_place = first_key + jnp.arange(key_heads.shape[0], dtype=jnp.int32)
    scores = jnp.einsum(
        "qhd,khd->hqk",
        query_block[..., :NOPE],
        key_heads[..., :NOPE],
        preferred_element_type=jnp.float32,
    )
    scores = scores + jnp.einsum(
        "qhd,kd->hqk", query_block[..., NOPE:], rope_keys, preferred_element_type=jnp.float32
    )
    scores = scores * (NOPE + ROPE) ** (-0.5)
    allowed = (key_place[None, :] >= starts[:, None]) & (key_place[None, :] <= places[:, None])
    return (jnp.where(allowed[None], scores, -jnp.inf), allowed)


def body(c_query, q_gain, w_query, kv_latent, kv_gain, w_kv, w_out, q_start):
    query_rows = c_query.shape[0]
    key_rows = kv_latent.shape[0]
    head_count = w_query.shape[1] // (NOPE + ROPE)
    block_index = lax.axis_index("seq")
    full_query = lax.all_gather(c_query, "head", axis=1, tiled=True)
    normed = rms_scale(full_query, q_gain).astype(jnp.bfloat16)
    query_raw = jnp.dot(normed, w_query, preferred_element_type=jnp.float32).reshape(
        query_rows, head_count, NOPE + ROPE
    )
    position = (
        block_index * key_rows + key_rows - query_rows + jnp.arange(query_rows, dtype=jnp.int32)
    )
    query_all = jnp.concatenate(
        [query_raw[..., :NOPE], rotate(query_raw[..., NOPE:], position)], axis=-1
    ).astype(jnp.bfloat16)
    kv_weights = lax.all_gather(w_kv, "seq", axis=1, tiled=True)

    def project(latent_block):
        scaled = rms_scale(latent_block, kv_gain).astype(jnp.bfloat16)
        return jnp.dot(scaled, kv_weights, preferred_element_type=jnp.float32).astype(jnp.bfloat16)

    own_heads = project(kv_latent[:, :KVL])
    own_rope = kv_latent[:, KVL:]
    head_parts = [own_heads]
    rope_parts = [own_rope]
    for offset in range(1, REACH + 1):
        moved_block = passed_along(kv_latent, "seq", offset)
        head_parts.insert(0, project(moved_block[:, :KVL]))
        rope_parts.insert(0, moved_block[:, KVL:])
    window_blocks = REACH + 1
    key_heads = jnp.concatenate(head_parts, axis=0).reshape(
        window_blocks * key_rows, head_count, NOPE + VDIM
    )
    rope_keys = jnp.concatenate(rope_parts, axis=0)
    scores, _ = masked_scores(
        query_all, q_start, position, key_heads, rope_keys, (block_index - REACH) * key_rows
    )
    largest = jnp.max(scores, axis=-1, keepdims=True)
    exponent_terms = jnp.exp(scores - largest)
    weights_bf = (exponent_terms / jnp.sum(exponent_terms, axis=-1, keepdims=True)).astype(
        jnp.bfloat16
    )
    attended = jnp.einsum(
        "hqk,khd->qhd", weights_bf, key_heads[..., NOPE:], preferred_element_type=jnp.float32
    )
    attended = attended.astype(jnp.bfloat16).reshape(query_rows, head_count * VDIM)
    partial_rows = jnp.dot(
        lax.all_gather(attended, "seq", axis=0, tiled=True),
        w_out,
        preferred_element_type=jnp.float32,
    )
    return lax.psum_scatter(partial_rows, "head", scatter_dimension=0, tiled=True).astype(
        jnp.bfloat16
    )


def exchanged(x, seq_flip, head_flip=0):
    if not head_flip:
        axes, flip, devices = "seq", seq_flip, lax.axis_size("seq")
    elif not seq_flip:
        axes, flip, devices = "head", head_flip, lax.axis_size("head")
    else:
        head = lax.axis_size("head")
        axes, flip = ("seq", "head"), seq_flip * head + head_flip
        devices = lax.axis_size("seq") * head
    return lax.ppermute(x, axes, [(i, i ^ flip) for i in range(devices)])


def pack_kernel(
    start_hbm, gain_hbm, query_hbm, latent_hbm, packed_ref, start_ref, gain_ref, query_ref, columns, sems
):
    rows = columns.shape[1]
    head_at = lax.axis_index("head")
    copy = pltpu.make_async_copy(
        latent_hbm.at[:, pl.ds(pl.multiple_of(head_at * rows, rows), rows)], columns, sems.at[0]
    )
    gain_copy = pltpu.make_async_copy(gain_hbm, gain_ref, sems.at[1])
    query_copy = pltpu.make_async_copy(query_hbm, query_ref, sems.at[2])
    start_copy = pltpu.make_async_copy(start_hbm, start_ref, sems.at[3])
    copies = (copy, gain_copy, query_copy, start_copy)
    for each in copies:
        each.start()
    for each in copies[1:]:
        each.wait()
    half = KVL // 2
    quarter = rows // 4
    query_rows = query_ref.shape[0]
    query_at = 2 * rows + quarter
    packed_ref[query_at : query_at + query_rows, :] = query_ref[:, :half]
    fold_at = query_at + query_rows
    folded = query_rows // 2
    packed_ref[fold_at : fold_at + folded, :] = jnp.concatenate(
        [query_ref[:folded, half:], query_ref[folded:, half:]], axis=1
    )
    start_at = fold_at + folded
    share = packed_ref.shape[0] - start_at
    window_first = (lax.axis_index("seq") - REACH) * (rows * (query_rows // share))
    shape = (share, half)
    row = lax.broadcasted_iota(jnp.int32, shape, 0)
    offset = jnp.zeros(shape, jnp.int32)
    for r in range(share):
        offset = jnp.where(row == r, start_ref[head_at * share + r] - window_first, offset)
    high = offset // DIGIT
    digit = jnp.where(
        lax.broadcasted_iota(jnp.int32, shape, 1) < half // 2, high, offset - high * DIGIT
    )
    packed_ref[start_at:, :] = digit.astype(jnp.float32).astype(jnp.bfloat16)
    copy.wait()
    values = columns[:KVL, :].astype(jnp.float32).T
    mean_square = jnp.mean(values * values, axis=-1, keepdims=True)
    normed = (values * lax.rsqrt(mean_square + EPS) * gain_ref[...]).astype(jnp.bfloat16)
    packed_ref[:rows, :] = normed[:, :half]
    packed_ref[rows : 2 * rows, :] = normed[:, half:]
    rope = columns[KVL:, :].astype(jnp.float32).T.astype(jnp.bfloat16)
    packed_ref[2 * rows : query_at, :] = jnp.concatenate(
        [rope[g * quarter : (g + 1) * quarter] for g in range(4)], axis=1
    )


def pack(kv_latent, kv_gain, c_query, q_start):
    head_devices = lax.axis_size("head")
    rows = kv_latent.shape[0] // head_devices
    query_rows = c_query.shape[0]
    packed_rows = 2 * rows + rows // 4 + query_rows + query_rows // 2 + query_rows // head_devices
    return pl.pallas_call(
        pack_kernel,
        out_shape=jax.ShapeDtypeStruct((packed_rows, KVL // 2), jnp.bfloat16),
        in_specs=[pl.BlockSpec(memory_space=pltpu.HBM)] * 4,
        out_specs=pl.BlockSpec(memory_space=pltpu.VMEM),
        scratch_shapes=[
            pltpu.SMEM(q_start.shape, jnp.int32),
            pltpu.VMEM((1, KVL), jnp.float32),
            pltpu.VMEM(c_query.shape, jnp.bfloat16),
            pltpu.VMEM((kv_latent.shape[1], rows), jnp.bfloat16),
            pltpu.SemaphoreType.DMA((4,)),
        ],
        name="pack",
    )(q_start, kv_gain.reshape(1, KVL), c_query, kv_latent.T)


HOPS = (
    ((0, 0), (4, 0)),
    ((0, 0), (2, 0)),
    ((0, 0), (1, 0)),
    ((0, 0), (0, 2)),
    ((1, 0), (0, 2)),
    ((2, 0), (1, 0)),
    ((2, 0), (0, 2)),
    ((4, 0), (2, 0)),
    ((4, 0), (1, 0)),
    ((4, 0), (0, 2)),
    ((2, 2), (1, 0)),
    ((6, 0), (1, 0)),
    ((6, 0), (0, 2)),
    ((5, 0), (0, 2)),
    ((6, 2), (1, 0)),
)


def gather_pieces(own):
    got = {(0, 0): own}
    for source, flip in HOPS:
        got[source[0] ^ flip[0], source[1] ^ flip[1]] = exchanged(got[source], *flip)
    for (seq_flip, head_flip), v in list(got.items()):
        got[seq_flip, head_flip + 1] = exchanged(v, 0, 1)
    return got


def stage_kernel(w_query_hbm, w_kv_hbm, gain_hbm, turn_hbm, w_query, w_kv, gain, turn, sems):
    columns = w_query.shape[1]
    left = pl.multiple_of(lax.axis_index("seq") * columns, 128)
    copies = (
        pltpu.make_async_copy(w_query_hbm.at[:, pl.ds(left, columns)], w_query, sems.at[0]),
        pltpu.make_async_copy(w_kv_hbm, w_kv, sems.at[1]),
        pltpu.make_async_copy(gain_hbm, gain, sems.at[2]),
        pltpu.make_async_copy(turn_hbm, turn, sems.at[3]),
    )
    for each in copies:
        each.start()
    for each in copies:
        each.wait()


def stage(w_query, w_kv, q_gain, turn):
    columns = w_kv.shape[1] // (NOPE + VDIM) * (NOPE + ROPE)
    vmem = pl.BlockSpec(memory_space=pltpu.VMEM)
    return pl.pallas_call(
        stage_kernel,
        out_shape=[
            jax.ShapeDtypeStruct((w_query.shape[0], columns), jnp.bfloat16),
            jax.ShapeDtypeStruct(w_kv.shape, jnp.bfloat16),
            jax.ShapeDtypeStruct(q_gain.shape, jnp.float32),
            jax.ShapeDtypeStruct(turn.shape, jnp.float32),
        ],
        in_specs=[pl.BlockSpec(memory_space=pltpu.HBM)] * 4,
        out_specs=[vmem] * 4,
        scratch_shapes=[pltpu.SemaphoreType.DMA((4,))],
        compiler_params=pltpu.CompilerParams(vmem_limit_bytes=STAGE_LIMIT),
        name="stage",
    )(w_query, w_kv, q_gain, turn)


def attend_kernel(flips, blocks, *refs):
    pieces = dict(zip(flips, refs[: len(flips)]))
    (w_query, w_kv_ref, gain_ref, turn_ref, out_ref) = refs[len(flips) : len(flips) + 5]
    (latent_query, starts, queries, keys, values, scores, probs) = refs[len(flips) + 5 :]
    seq_at = lax.axis_index("seq")
    head_at = lax.axis_index("head")
    parts = len(flips) // blocks
    heads = queries.shape[0]
    wide = NOPE + ROPE
    query_rows = queries.shape[1] // blocks
    key_rows = keys.shape[1] // blocks
    rows = key_rows // parts
    half = KVL // 2
    quarter = rows // 4
    rope_at = 2 * rows
    query_at = rope_at + quarter
    fold_at = query_at + query_rows
    folded = query_rows // 2
    start_at = fold_at + folded
    share = query_rows // parts
    query_wide = latent_query.shape[1] // parts
    rest = query_wide - half
    for seq_flip in range(blocks):
        top = pl.multiple_of((seq_at ^ seq_flip) * query_rows, query_rows)
        for f in range(parts):
            piece = pieces[seq_flip, f]
            part = head_at ^ f
            at = pl.multiple_of(part * query_wide, 128)
            latent_query[pl.ds(top, query_rows), pl.ds(at, half)] = piece[query_at:fold_at, :]
            at = pl.multiple_of(at + half, 128)
            for g in range(2):
                latent_query[pl.ds(top + g * folded, folded), pl.ds(at, rest)] = piece[
                    fold_at:start_at, g * rest : (g + 1) * rest
                ]
            to = pl.multiple_of(top + part * share, share)
            starts[pl.ds(to, share), :] = piece[start_at:, :].astype(jnp.float32)

    for seq_flip in range(blocks):
        key_top = pl.multiple_of((seq_at ^ seq_flip) * key_rows, key_rows)
        low = jnp.concatenate([pieces[seq_flip, f][:rows, :] for f in range(parts)], axis=0)
        high = jnp.concatenate(
            [pieces[seq_flip, f][rows : 2 * rows, :] for f in range(parts)], axis=0
        )
        both = jnp.dot(low, w_kv_ref[:half, :], preferred_element_type=jnp.float32) + jnp.dot(
            high, w_kv_ref[half:, :], preferred_element_type=jnp.float32
        )
        both = both.astype(jnp.bfloat16)
        for f in range(parts):
            piece = pieces[seq_flip, f]
            to = pl.multiple_of(key_top + (head_at ^ f) * rows, rows)
            span = slice(f * rows, (f + 1) * rows)
            rope = jnp.concatenate(
                [piece[rope_at:query_at, g * ROPE : (g + 1) * ROPE] for g in range(4)], axis=0
            )
            for j in range(heads):
                left = j * (NOPE + VDIM)
                keys[j, pl.ds(to, rows), :NOPE] = both[span, left : left + NOPE]
                keys[j, pl.ds(to, rows), NOPE:] = rope
                values[j, pl.ds(to, rows), :] = both[span, left + NOPE : left + NOPE + VDIM]

    for b in range(blocks):
        span = slice(b * query_rows, (b + 1) * query_rows)
        wide_rows = latent_query[span, :].astype(jnp.float32)
        mean_square = jnp.mean(wide_rows * wide_rows, axis=-1, keepdims=True)
        latent_query[span, :] = (
            wide_rows * lax.rsqrt(mean_square + EPS) * gain_ref[...].reshape(1, -1)
        ).astype(jnp.bfloat16)
    raw = jnp.dot(latent_query[...], w_query[...], preferred_element_type=jnp.float32)
    for j in range(heads):
        head_raw = raw[:, j * wide : (j + 1) * wide]
        queries[j, :, :NOPE] = head_raw[:, :NOPE].astype(jnp.bfloat16)
        rotary = head_raw[:, NOPE:]
        crossed = jnp.concatenate([rotary[:, ROPE // 2 :], rotary[:, : ROPE // 2]], axis=1)
        queries[j, :, NOPE:] = (
            rotary * turn_ref[:, :ROPE] + crossed * turn_ref[:, ROPE:]
        ).astype(jnp.bfloat16)

    def score(b):
        count = min(REACH + 1, blocks - b) * query_rows
        for j in range(heads):
            scores[j, b, :count, :] = lax.dot_general(
                queries[j, b * query_rows : b * query_rows + count, :],
                keys[j, b * key_rows : (b + 1) * key_rows, :],
                (((1,), (1,)), ((), ())),
                preferred_element_type=jnp.float32,
            )

    def soften(b):
        digits = starts[b * query_rows : (b + 1) * query_rows, :]
        offset = digits[:, :128] * DIGIT + digits[:, half // 2 : half // 2 + 128]
        start = jnp.concatenate([offset] * (key_rows // 128), axis=1).astype(jnp.int32)
        window = range(max(b - REACH, 0), b + 1)
        shape = (query_rows, key_rows)
        column = lax.broadcasted_iota(jnp.int32, shape, 1)
        row = lax.broadcasted_iota(jnp.int32, shape, 0)
        for j in range(heads):
            masked = []
            for w in window:
                top = (b - w) * query_rows
                part = scores[j, w, top : top + query_rows, :] * wide ** (-0.5)
                allowed = column >= start - (w - b + REACH) * key_rows
                if w == b:
                    allowed = allowed & (column <= row + (key_rows - query_rows))
                masked.append(jnp.where(allowed, part, -jnp.inf))
            largest = masked[0]
            for part in masked[1:]:
                largest = jnp.maximum(largest, part)
            largest = jnp.max(largest, axis=-1, keepdims=True)
            terms = [jnp.exp(part - largest) for part in masked]
            total = terms[0]
            for part in terms[1:]:
                total = total + part
            inverse = 1.0 / jnp.sum(total, axis=-1, keepdims=True)
            for w, part in zip(window, terms):
                top = (b - w) * query_rows
                probs[j, w, top : top + query_rows, :] = (part * inverse).astype(jnp.bfloat16)

    for b in range(blocks):
        score(b)
        soften(b)
    for j in range(heads):
        sums = [None] * blocks
        for w in range(blocks):
            count = min(REACH + 1, blocks - w)
            mixed = jnp.dot(
                probs[j, w, : count * query_rows, :],
                values[j, w * key_rows : (w + 1) * key_rows, :],
                preferred_element_type=jnp.float32,
            )
            for i in range(count):
                part = mixed[i * query_rows : (i + 1) * query_rows]
                sums[w + i] = part if sums[w + i] is None else sums[w + i] + part
            out_ref[w * query_rows : (w + 1) * query_rows, j * VDIM : (j + 1) * VDIM] = sums[
                w
            ].astype(jnp.bfloat16)


def attend(got, weights, query_rows, key_rows):
    blocks = lax.axis_size("seq")
    w_query, w_kv, _, _ = weights
    flips = tuple(sorted(got))
    pieces = [got[f] for f in flips]
    heads = w_kv.shape[1] // (NOPE + VDIM)
    wide = NOPE + ROPE
    queries = blocks * query_rows
    keys = key_rows * blocks
    count = (REACH + 1) * query_rows
    vmem = pl.BlockSpec(memory_space=pltpu.VMEM)
    return pl.pallas_call(
        functools.partial(attend_kernel, flips, blocks),
        out_shape=jax.ShapeDtypeStruct((queries, heads * VDIM), jnp.bfloat16),
        in_specs=[vmem] * (len(flips) + len(weights)),
        out_specs=vmem,
        scratch_shapes=[
            pltpu.VMEM((queries, w_query.shape[0]), jnp.bfloat16),
            pltpu.VMEM((queries, KVL // 2), jnp.float32),
            pltpu.VMEM((heads, queries, wide), jnp.bfloat16),
            pltpu.VMEM((heads, keys, wide), jnp.bfloat16),
            pltpu.VMEM((heads, keys, VDIM), jnp.bfloat16),
            pltpu.VMEM((heads, blocks, count, key_rows), jnp.float32),
            pltpu.VMEM((heads, blocks, count, key_rows), jnp.bfloat16),
        ],
        compiler_params=pltpu.CompilerParams(vmem_limit_bytes=32 << 20),
        name="attend",
    )(*pieces, *weights)


def project_out_kernel(blocks, *refs):
    pieces = refs[:blocks]
    w_out_ref = refs[blocks]
    outs = refs[blocks + 1 : -1]
    summed = refs[-1]
    seq_at = lax.axis_index("seq")
    head_at = lax.axis_index("head")
    features = pieces[0].shape[1]
    columns = w_out_ref.shape[1]
    for left in range(0, columns, 256):
        span = slice(left, min(left + 256, columns))
        total = None
        for flip in range(blocks):
            top = pl.multiple_of((seq_at ^ flip) * features, features)
            part = jnp.dot(
                pieces[flip][...],
                w_out_ref[pl.ds(top, features), span],
                preferred_element_type=jnp.float32,
            )
            total = part if total is None else total + part
        summed[:, span] = total
    rows = outs[0].shape[0]
    for flip, out_ref in enumerate(outs):
        top = pl.multiple_of((head_at ^ flip) * rows, rows)
        out_ref[...] = summed[pl.ds(top, rows), :].astype(out_ref.dtype)


def project_out(pieces, w_out):
    owners = lax.axis_size("head")
    queries = pieces[0].shape[0]
    columns = w_out.shape[1]
    vmem = pl.BlockSpec(memory_space=pltpu.VMEM)
    return pl.pallas_call(
        functools.partial(project_out_kernel, len(pieces)),
        out_shape=[
            jax.ShapeDtypeStruct((queries // owners, columns), jnp.bfloat16 if k else jnp.float32)
            for k in range(owners)
        ],
        in_specs=[vmem] * (len(pieces) + 1),
        out_specs=[vmem] * owners,
        scratch_shapes=[pltpu.VMEM((queries, columns), jnp.float32)],
        compiler_params=pltpu.CompilerParams(vmem_limit_bytes=16 << 20),
        name="project_out",
    )(*pieces, w_out)


SPREAD_HOPS = ((0, 4), (0, 1), (0, 2), (1, 2), (4, 2), (4, 1), (4, 3))


def rotation_table(blocks, query_rows, key_rows):
    serial = np.arange(blocks * query_rows)
    position = serial // query_rows * key_rows + key_rows - query_rows + serial % query_rows
    angles = position[:, None] * THETA ** (-np.arange(ROPE // 2) * (2.0 / ROPE))[None, :]
    cosine, sine_of = np.cos(angles), np.sin(angles)
    return np.concatenate([cosine, cosine, -sine_of, sine_of], axis=1).astype(np.float32)


def heads_body(c_query, q_gain, w_query, kv_latent, kv_gain, w_kv, w_out, q_start):
    blocks = lax.axis_size("seq")
    query_rows = c_query.shape[0]
    key_rows = kv_latent.shape[0]
    own = pack(kv_latent, kv_gain, c_query, q_start)
    weights = stage(w_query, w_kv, q_gain, rotation_table(blocks, query_rows, key_rows))
    got = gather_pieces(own)
    attended = attend(got, weights, query_rows, key_rows)
    spread = {0: attended}
    for source, flip in SPREAD_HOPS:
        spread[source ^ flip] = exchanged(spread[source], flip)
    shares = project_out([spread[k] for k in range(blocks)], w_out)
    total = shares[0]
    for k in range(1, len(shares)):
        total = total + exchanged(shares[k], 0, k).astype(jnp.float32)
    return total.astype(jnp.bfloat16)


def solution(mesh):
    in_specs = (
        P("seq", "head"),
        P(),
        P(None, "head"),
        P("seq", None),
        P(),
        P(None, ("head", "seq")),
        P("head", "seq"),
        P("seq"),
    )
    out_specs = P("head", "seq")

    def layer(*args):
        _, _, _, _, _, w_kv, _, _ = args
        seq, heads = mesh.shape["seq"], mesh.shape["head"]
        own_columns = w_kv.shape[1] // (seq * heads)
        whole_heads = own_columns % (NOPE + VDIM) == 0
        by_heads = whole_heads and (seq, heads) == (8, 4)
        step = jax.shard_map(
            heads_body if by_heads else body,
            mesh=mesh,
            in_specs=in_specs,
            out_specs=out_specs,
            check_vma=False,
        )
        return step(*args)

    return layer
```

```python
import functools

import jax
import jax.numpy as jnp
import numpy as np
from jax import lax
from jax.experimental import pallas as pl
from jax.experimental.pallas import tpu as pltpu
from jax.sharding import PartitionSpec as P


KVL = 512
NOPE = 128
ROPE = 64
VDIM = 128
REACH = 3
DIGIT = 64
STAGE_LIMIT = 52000 << 10


EPS = 1e-06
THETA = 10000.0


def passed_along(x, axis, by):
    devices = lax.axis_size(axis)
    pairs = [(i, i + by) for i in range(devices) if 0 <= i + by < devices]
    return lax.ppermute(x, axis, pairs)


def rms_scale(latent_rows, gain_row):
    values = latent_rows.astype(jnp.float32)
    mean_square = jnp.mean(values * values, axis=-1, keepdims=True)
    return values * lax.rsqrt(mean_square + EPS) * gain_row


def rotate(rotary, position):
    half_size = rotary.shape[-1] // 2
    exponent = jnp.arange(half_size, dtype=jnp.float32) * (2.0 / rotary.shape[-1])
    angles = position.astype(jnp.float32)[:, None] * (THETA ** (-exponent))[None, :]
    cosine = jnp.cos(angles)[:, None, :]
    sine_of = jnp.sin(angles)[:, None, :]
    former = rotary[..., :half_size]
    latter = rotary[..., half_size:]
    return jnp.concatenate(
        [former * cosine - latter * sine_of, latter * cosine + former * sine_of], axis=-1
    )


def masked_scores(query_block, starts, places, key_heads, rope_keys, first_key):
    key_place = first_key + jnp.arange(key_heads.shape[0], dtype=jnp.int32)
    scores = jnp.einsum(
        "qhd,khd->hqk",
        query_block[..., :NOPE],
        key_heads[..., :NOPE],
        preferred_element_type=jnp.float32,
    )
    scores = scores + jnp.einsum(
        "qhd,kd->hqk", query_block[..., NOPE:], rope_keys, preferred_element_type=jnp.float32
    )
    scores = scores * (NOPE + ROPE) ** (-0.5)
    allowed = (key_place[None, :] >= starts[:, None]) & (key_place[None, :] <= places[:, None])
    return (jnp.where(allowed[None], scores, -jnp.inf), allowed)


def body(c_query, q_gain, w_query, kv_latent, kv_gain, w_kv, w_out, q_start):
    query_rows = c_query.shape[0]
    key_rows = kv_latent.shape[0]
    head_count = w_query.shape[1] // (NOPE + ROPE)
    block_index = lax.axis_index("seq")
    full_query = lax.all_gather(c_query, "head", axis=1, tiled=True)
    normed = rms_scale(full_query, q_gain).astype(jnp.bfloat16)
    query_raw = jnp.dot(normed, w_query, preferred_element_type=jnp.float32).reshape(
        query_rows, head_count, NOPE + ROPE
    )
    position = (
        block_index * key_rows + key_rows - query_rows + jnp.arange(query_rows, dtype=jnp.int32)
    )
    query_all = jnp.concatenate(
        [query_raw[..., :NOPE], rotate(query_raw[..., NOPE:], position)], axis=-1
    ).astype(jnp.bfloat16)
    kv_weights = lax.all_gather(w_kv, "seq", axis=1, tiled=True)

    def project(latent_block):
        scaled = rms_scale(latent_block, kv_gain).astype(jnp.bfloat16)
        return jnp.dot(scaled, kv_weights, preferred_element_type=jnp.float32).astype(jnp.bfloat16)

    own_heads = project(kv_latent[:, :KVL])
    own_rope = kv_latent[:, KVL:]
    head_parts = [own_heads]
    rope_parts = [own_rope]
    for offset in range(1, REACH + 1):
        moved_block = passed_along(kv_latent, "seq", offset)
        head_parts.insert(0, project(moved_block[:, :KVL]))
        rope_parts.insert(0, moved_block[:, KVL:])
    window_blocks = REACH + 1
    key_heads = jnp.concatenate(head_parts, axis=0).reshape(
        window_blocks * key_rows, head_count, NOPE + VDIM
    )
    rope_keys = jnp.concatenate(rope_parts, axis=0)
    scores, _ = masked_scores(
        query_all, q_start, position, key_heads, rope_keys, (block_index - REACH) * key_rows
    )
    largest = jnp.max(scores, axis=-1, keepdims=True)
    exponent_terms = jnp.exp(scores - largest)
    weights_bf = (exponent_terms / jnp.sum(exponent_terms, axis=-1, keepdims=True)).astype(
        jnp.bfloat16
    )
    attended = jnp.einsum(
        "hqk,khd->qhd", weights_bf, key_heads[..., NOPE:], preferred_element_type=jnp.float32
    )
    attended = attended.astype(jnp.bfloat16).reshape(query_rows, head_count * VDIM)
    partial_rows = jnp.dot(
        lax.all_gather(attended, "seq", axis=0, tiled=True),
        w_out,
        preferred_element_type=jnp.float32,
    )
    return lax.psum_scatter(partial_rows, "head", scatter_dimension=0, tiled=True).astype(
        jnp.bfloat16
    )


def exchanged(x, seq_flip, head_flip=0):
    if not head_flip:
        axes, flip, devices = "seq", seq_flip, lax.axis_size("seq")
    elif not seq_flip:
        axes, flip, devices = "head", head_flip, lax.axis_size("head")
    else:
        head = lax.axis_size("head")
        axes, flip = ("seq", "head"), seq_flip * head + head_flip
        devices = lax.axis_size("seq") * head
    return lax.ppermute(x, axes, [(i, i ^ flip) for i in range(devices)])


def pack_kernel(
    start_hbm, gain_hbm, query_hbm, latent_hbm, packed_ref, start_ref, gain_ref, query_ref, columns, sems
):
    rows = columns.shape[1]
    head_at = lax.axis_index("head")
    copy = pltpu.make_async_copy(
        latent_hbm.at[:, pl.ds(pl.multiple_of(head_at * rows, rows), rows)], columns, sems.at[0]
    )
    gain_copy = pltpu.make_async_copy(gain_hbm, gain_ref, sems.at[1])
    query_copy = pltpu.make_async_copy(query_hbm, query_ref, sems.at[2])
    start_copy = pltpu.make_async_copy(start_hbm, start_ref, sems.at[3])
    copies = (copy, gain_copy, query_copy, start_copy)
    for each in copies:
        each.start()
    for each in copies[1:]:
        each.wait()
    half = KVL // 2
    quarter = rows // 4
    query_rows = query_ref.shape[0]
    query_at = 2 * rows + quarter
    packed_ref[query_at : query_at + query_rows, :] = query_ref[:, :half]
    fold_at = query_at + query_rows
    folded = query_rows // 2
    packed_ref[fold_at : fold_at + folded, :] = jnp.concatenate(
        [query_ref[:folded, half:], query_ref[folded:, half:]], axis=1
    )
    start_at = fold_at + folded
    share = packed_ref.shape[0] - start_at
    window_first = (lax.axis_index("seq") - REACH) * (rows * (query_rows // share))
    shape = (share, half)
    row = lax.broadcasted_iota(jnp.int32, shape, 0)
    offset = jnp.zeros(shape, jnp.int32)
    for r in range(share):
        offset = jnp.where(row == r, start_ref[head_at * share + r] - window_first, offset)
    high = offset // DIGIT
    digit = jnp.where(
        lax.broadcasted_iota(jnp.int32, shape, 1) < half // 2, high, offset - high * DIGIT
    )
    packed_ref[start_at:, :] = digit.astype(jnp.float32).astype(jnp.bfloat16)
    copy.wait()
    values = columns[:KVL, :].astype(jnp.float32).T
    mean_square = jnp.mean(values * values, axis=-1, keepdims=True)
    normed = (values * lax.rsqrt(mean_square + EPS) * gain_ref[...]).astype(jnp.bfloat16)
    packed_ref[:rows, :] = normed[:, :half]
    packed_ref[rows : 2 * rows, :] = normed[:, half:]
    rope = columns[KVL:, :].astype(jnp.float32).T.astype(jnp.bfloat16)
    packed_ref[2 * rows : query_at, :] = jnp.concatenate(
        [rope[g * quarter : (g + 1) * quarter] for g in range(4)], axis=1
    )


def pack(kv_latent, kv_gain, c_query, q_start):
    head_devices = lax.axis_size("head")
    rows = kv_latent.shape[0] // head_devices
    query_rows = c_query.shape[0]
    packed_rows = 2 * rows + rows // 4 + query_rows + query_rows // 2 + query_rows // head_devices
    return pl.pallas_call(
        pack_kernel,
        out_shape=jax.ShapeDtypeStruct((packed_rows, KVL // 2), jnp.bfloat16),
        in_specs=[pl.BlockSpec(memory_space=pltpu.HBM)] * 4,
        out_specs=pl.BlockSpec(memory_space=pltpu.VMEM),
        scratch_shapes=[
            pltpu.SMEM(q_start.shape, jnp.int32),
            pltpu.VMEM((1, KVL), jnp.float32),
            pltpu.VMEM(c_query.shape, jnp.bfloat16),
            pltpu.VMEM((kv_latent.shape[1], rows), jnp.bfloat16),
            pltpu.SemaphoreType.DMA((4,)),
        ],
        name="pack",
    )(q_start, kv_gain.reshape(1, KVL), c_query, kv_latent.T)


HOPS = (
    ((0, 0), (2, 0)),
    ((0, 0), (4, 0)),
    ((0, 0), (1, 0)),
    ((0, 0), (0, 2)),
    ((2, 0), (1, 0)),
    ((2, 0), (0, 2)),
    ((1, 0), (0, 2)),
    ((4, 0), (1, 0)),
    ((4, 0), (0, 2)),
    ((4, 0), (2, 0)),
    ((2, 2), (1, 0)),
    ((5, 0), (2, 0)),
    ((4, 2), (2, 0)),
    ((5, 0), (0, 2)),
    ((6, 0), (1, 2)),
)


def gather_pieces(own):
    got = {(0, 0): own}
    for source, flip in HOPS:
        got[source[0] ^ flip[0], source[1] ^ flip[1]] = exchanged(got[source], *flip)
    for (seq_flip, head_flip), v in list(got.items()):
        got[seq_flip, head_flip + 1] = exchanged(v, 0, 1)
    return got


def stage_kernel(w_query_hbm, w_kv_hbm, gain_hbm, turn_hbm, w_query, w_kv, gain, turn, sems):
    columns = w_query.shape[1]
    left = pl.multiple_of(lax.axis_index("seq") * columns, 128)
    copies = (
        pltpu.make_async_copy(w_query_hbm.at[:, pl.ds(left, columns)], w_query, sems.at[0]),
        pltpu.make_async_copy(w_kv_hbm, w_kv, sems.at[1]),
        pltpu.make_async_copy(gain_hbm, gain, sems.at[2]),
        pltpu.make_async_copy(turn_hbm, turn, sems.at[3]),
    )
    for each in copies:
        each.start()
    for each in copies:
        each.wait()


def stage(w_query, w_kv, q_gain, turn):
    columns = w_kv.shape[1] // (NOPE + VDIM) * (NOPE + ROPE)
    vmem = pl.BlockSpec(memory_space=pltpu.VMEM)
    return pl.pallas_call(
        stage_kernel,
        out_shape=[
            jax.ShapeDtypeStruct((w_query.shape[0], columns), jnp.bfloat16),
            jax.ShapeDtypeStruct(w_kv.shape, jnp.bfloat16),
            jax.ShapeDtypeStruct(q_gain.shape, jnp.float32),
            jax.ShapeDtypeStruct(turn.shape, jnp.float32),
        ],
        in_specs=[pl.BlockSpec(memory_space=pltpu.HBM)] * 4,
        out_specs=[vmem] * 4,
        scratch_shapes=[pltpu.SemaphoreType.DMA((4,))],
        compiler_params=pltpu.CompilerParams(vmem_limit_bytes=STAGE_LIMIT),
        name="stage",
    )(w_query, w_kv, q_gain, turn)


def attend_kernel(flips, blocks, *refs):
    pieces = dict(zip(flips, refs[: len(flips)]))
    (w_query, w_kv_ref, gain_ref, turn_ref, out_ref) = refs[len(flips) : len(flips) + 5]
    (latent_query, starts, queries, keys, values, scores, probs) = refs[len(flips) + 5 :]
    seq_at = lax.axis_index("seq")
    head_at = lax.axis_index("head")
    parts = len(flips) // blocks
    heads = queries.shape[0]
    wide = NOPE + ROPE
    query_rows = queries.shape[1] // blocks
    key_rows = keys.shape[1] // blocks
    rows = key_rows // parts
    half = KVL // 2
    quarter = rows // 4
    rope_at = 2 * rows
    query_at = rope_at + quarter
    fold_at = query_at + query_rows
    folded = query_rows // 2
    start_at = fold_at + folded
    share = query_rows // parts
    query_wide = latent_query.shape[1] // parts
    rest = query_wide - half
    for seq_flip in range(blocks):
        top = pl.multiple_of((seq_at ^ seq_flip) * query_rows, query_rows)
        for f in range(parts):
            piece = pieces[seq_flip, f]
            part = head_at ^ f
            at = pl.multiple_of(part * query_wide, 128)
            latent_query[pl.ds(top, query_rows), pl.ds(at, half)] = piece[query_at:fold_at, :]
            at = pl.multiple_of(at + half, 128)
            for g in range(2):
                latent_query[pl.ds(top + g * folded, folded), pl.ds(at, rest)] = piece[
                    fold_at:start_at, g * rest : (g + 1) * rest
                ]
            to = pl.multiple_of(top + part * share, share)
            starts[pl.ds(to, share), :] = piece[start_at:, :].astype(jnp.float32)

    for seq_flip in range(blocks):
        key_top = pl.multiple_of((seq_at ^ seq_flip) * key_rows, key_rows)
        low = jnp.concatenate([pieces[seq_flip, f][:rows, :] for f in range(parts)], axis=0)
        high = jnp.concatenate(
            [pieces[seq_flip, f][rows : 2 * rows, :] for f in range(parts)], axis=0
        )
        both = jnp.dot(low, w_kv_ref[:half, :], preferred_element_type=jnp.float32) + jnp.dot(
            high, w_kv_ref[half:, :], preferred_element_type=jnp.float32
        )
        both = both.astype(jnp.bfloat16)
        for f in range(parts):
            piece = pieces[seq_flip, f]
            to = pl.multiple_of(key_top + (head_at ^ f) * rows, rows)
            span = slice(f * rows, (f + 1) * rows)
            rope = jnp.concatenate(
                [piece[rope_at:query_at, g * ROPE : (g + 1) * ROPE] for g in range(4)], axis=0
            )
            for j in range(heads):
                left = j * (NOPE + VDIM)
                keys[j, pl.ds(to, rows), :NOPE] = both[span, left : left + NOPE]
                keys[j, pl.ds(to, rows), NOPE:] = rope
                values[j, pl.ds(to, rows), :] = both[span, left + NOPE : left + NOPE + VDIM]

    for b in range(blocks):
        span = slice(b * query_rows, (b + 1) * query_rows)
        wide_rows = latent_query[span, :].astype(jnp.float32)
        mean_square = jnp.mean(wide_rows * wide_rows, axis=-1, keepdims=True)
        latent_query[span, :] = (
            wide_rows * lax.rsqrt(mean_square + EPS) * gain_ref[...].reshape(1, -1)
        ).astype(jnp.bfloat16)
    raw = jnp.dot(latent_query[...], w_query[...], preferred_element_type=jnp.float32)
    for j in range(heads):
        head_raw = raw[:, j * wide : (j + 1) * wide]
        queries[j, :, :NOPE] = head_raw[:, :NOPE].astype(jnp.bfloat16)
        rotary = head_raw[:, NOPE:]
        crossed = jnp.concatenate([rotary[:, ROPE // 2 :], rotary[:, : ROPE // 2]], axis=1)
        queries[j, :, NOPE:] = (
            rotary * turn_ref[:, :ROPE] + crossed * turn_ref[:, ROPE:]
        ).astype(jnp.bfloat16)

    def score(b):
        count = min(REACH + 1, blocks - b) * query_rows
        for j in range(heads):
            scores[j, b, :count, :] = lax.dot_general(
                queries[j, b * query_rows : b * query_rows + count, :],
                keys[j, b * key_rows : (b + 1) * key_rows, :],
                (((1,), (1,)), ((), ())),
                preferred_element_type=jnp.float32,
            )

    def soften(b):
        digits = starts[b * query_rows : (b + 1) * query_rows, :]
        offset = digits[:, :128] * DIGIT + digits[:, half // 2 : half // 2 + 128]
        start = jnp.concatenate([offset] * (key_rows // 128), axis=1).astype(jnp.int32)
        window = range(max(b - REACH, 0), b + 1)
        shape = (query_rows, key_rows)
        column = lax.broadcasted_iota(jnp.int32, shape, 1)
        row = lax.broadcasted_iota(jnp.int32, shape, 0)
        for j in range(heads):
            masked = []
            for w in window:
                top = (b - w) * query_rows
                part = scores[j, w, top : top + query_rows, :] * wide ** (-0.5)
                allowed = column >= start - (w - b + REACH) * key_rows
                if w == b:
                    allowed = allowed & (column <= row + (key_rows - query_rows))
                masked.append(jnp.where(allowed, part, -jnp.inf))
            largest = masked[0]
            for part in masked[1:]:
                largest = jnp.maximum(largest, part)
            largest = jnp.max(largest, axis=-1, keepdims=True)
            terms = [jnp.exp(part - largest) for part in masked]
            total = terms[0]
            for part in terms[1:]:
                total = total + part
            inverse = 1.0 / jnp.sum(total, axis=-1, keepdims=True)
            for w, part in zip(window, terms):
                top = (b - w) * query_rows
                probs[j, w, top : top + query_rows, :] = (part * inverse).astype(jnp.bfloat16)

    for b in range(blocks):
        score(b)
        soften(b)
    for j in range(heads):
        sums = [None] * blocks
        for w in range(blocks):
            count = min(REACH + 1, blocks - w)
            mixed = jnp.dot(
                probs[j, w, : count * query_rows, :],
                values[j, w * key_rows : (w + 1) * key_rows, :],
                preferred_element_type=jnp.float32,
            )
            for i in range(count):
                part = mixed[i * query_rows : (i + 1) * query_rows]
                sums[w + i] = part if sums[w + i] is None else sums[w + i] + part
            out_ref[w * query_rows : (w + 1) * query_rows, j * VDIM : (j + 1) * VDIM] = sums[
                w
            ].astype(jnp.bfloat16)


def attend(got, weights, query_rows, key_rows):
    blocks = lax.axis_size("seq")
    w_query, w_kv, _, _ = weights
    flips = tuple(sorted(got))
    pieces = [got[f] for f in flips]
    heads = w_kv.shape[1] // (NOPE + VDIM)
    wide = NOPE + ROPE
    queries = blocks * query_rows
    keys = key_rows * blocks
    count = (REACH + 1) * query_rows
    vmem = pl.BlockSpec(memory_space=pltpu.VMEM)
    return pl.pallas_call(
        functools.partial(attend_kernel, flips, blocks),
        out_shape=jax.ShapeDtypeStruct((queries, heads * VDIM), jnp.bfloat16),
        in_specs=[vmem] * (len(flips) + len(weights)),
        out_specs=vmem,
        scratch_shapes=[
            pltpu.VMEM((queries, w_query.shape[0]), jnp.bfloat16),
            pltpu.VMEM((queries, KVL // 2), jnp.float32),
            pltpu.VMEM((heads, queries, wide), jnp.bfloat16),
            pltpu.VMEM((heads, keys, wide), jnp.bfloat16),
            pltpu.VMEM((heads, keys, VDIM), jnp.bfloat16),
            pltpu.VMEM((heads, blocks, count, key_rows), jnp.float32),
            pltpu.VMEM((heads, blocks, count, key_rows), jnp.bfloat16),
        ],
        compiler_params=pltpu.CompilerParams(vmem_limit_bytes=32 << 20),
        name="attend",
    )(*pieces, *weights)


def project_out_kernel(blocks, *refs):
    pieces = refs[:blocks]
    w_out_ref = refs[blocks]
    outs = refs[blocks + 1 : -1]
    summed = refs[-1]
    seq_at = lax.axis_index("seq")
    head_at = lax.axis_index("head")
    features = pieces[0].shape[1]
    columns = w_out_ref.shape[1]
    for left in range(0, columns, 256):
        span = slice(left, min(left + 256, columns))
        total = None
        for flip in range(blocks):
            top = pl.multiple_of((seq_at ^ flip) * features, features)
            part = jnp.dot(
                pieces[flip][...],
                w_out_ref[pl.ds(top, features), span],
                preferred_element_type=jnp.float32,
            )
            total = part if total is None else total + part
        summed[:, span] = total
    rows = outs[0].shape[0]
    for flip, out_ref in enumerate(outs):
        top = pl.multiple_of((head_at ^ flip) * rows, rows)
        out_ref[...] = summed[pl.ds(top, rows), :].astype(out_ref.dtype)


def project_out(pieces, w_out):
    owners = lax.axis_size("head")
    queries = pieces[0].shape[0]
    columns = w_out.shape[1]
    vmem = pl.BlockSpec(memory_space=pltpu.VMEM)
    return pl.pallas_call(
        functools.partial(project_out_kernel, len(pieces)),
        out_shape=[
            jax.ShapeDtypeStruct((queries // owners, columns), jnp.bfloat16 if k else jnp.float32)
            for k in range(owners)
        ],
        in_specs=[vmem] * (len(pieces) + 1),
        out_specs=[vmem] * owners,
        scratch_shapes=[pltpu.VMEM((queries, columns), jnp.float32)],
        compiler_params=pltpu.CompilerParams(vmem_limit_bytes=16 << 20),
        name="project_out",
    )(*pieces, w_out)


SPREAD_HOPS = ((0, 4), (0, 2), (0, 1), (2, 1), (4, 2), (4, 1), (4, 3))


def rotation_table(blocks, query_rows, key_rows):
    serial = np.arange(blocks * query_rows)
    position = serial // query_rows * key_rows + key_rows - query_rows + serial % query_rows
    angles = position[:, None] * THETA ** (-np.arange(ROPE // 2) * (2.0 / ROPE))[None, :]
    cosine, sine_of = np.cos(angles), np.sin(angles)
    return np.concatenate([cosine, cosine, -sine_of, sine_of], axis=1).astype(np.float32)


def heads_body(c_query, q_gain, w_query, kv_latent, kv_gain, w_kv, w_out, q_start):
    blocks = lax.axis_size("seq")
    query_rows = c_query.shape[0]
    key_rows = kv_latent.shape[0]
    own = pack(kv_latent, kv_gain, c_query, q_start)
    weights = stage(w_query, w_kv, q_gain, rotation_table(blocks, query_rows, key_rows))
    got = gather_pieces(own)
    attended = attend(got, weights, query_rows, key_rows)
    spread = {0: attended}
    for source, flip in SPREAD_HOPS:
        spread[source ^ flip] = exchanged(spread[source], flip)
    shares = project_out([spread[k] for k in range(blocks)], w_out)
    total = shares[0]
    for k in range(1, len(shares)):
        total = total + exchanged(shares[k], 0, k).astype(jnp.float32)
    return total.astype(jnp.bfloat16)


def solution(mesh):
    in_specs = (
        P("seq", "head"),
        P(),
        P(None, "head"),
        P("seq", None),
        P(),
        P(None, ("head", "seq")),
        P("head", "seq"),
        P("seq"),
    )
    out_specs = P("head", "seq")

    def layer(*args):
        _, _, _, _, _, w_kv, _, _ = args
        seq, heads = mesh.shape["seq"], mesh.shape["head"]
        own_columns = w_kv.shape[1] // (seq * heads)
        whole_heads = own_columns % (NOPE + VDIM) == 0
        by_heads = whole_heads and (seq, heads) == (8, 4)
        step = jax.shard_map(
            heads_body if by_heads else body,
            mesh=mesh,
            in_specs=in_specs,
            out_specs=out_specs,
            check_vma=False,
        )
        return step(*args)

    return layer
```
